256 devices in a mesh: dp: 32 (over z_hi, y, core), tensor: 8 (over z_lo, x).
Axes of the slice: x: 4, y: 4, z: 8 (z_hi: 4, z_lo: 2; z = z_hi * 2 + z_lo), core: 2. Of those that a mesh axis runs over, the one named last changes fastest.
Arguments:
- tokens: bfloat16 [8192, 2560], P('dp'), may hold values from -6 to 6
- target: bfloat16 [8192, 2560], P('dp'), may hold values from -6 to 6
- norm_gain: float32 [2560], replicated, may hold values from 0.25 to 1.75
- gate_weight: bfloat16 [2560, 7168], P('dp', 'tensor'), may hold values from -0.125 to 0.125
- up_weight: bfloat16 [2560, 7168], P('dp', 'tensor'), may hold values from -0.125 to 0.125
- down_weight: bfloat16 [7168, 2560], P('tensor', 'dp'), may hold values from -0.0625 to 0.0625
- tangent: bfloat16 [2560, 7168], P('dp', 'tensor'), may hold values from -0.125 to 0.125
- lengths: int32 [4], replicated, may hold values from 512 to 2048
- loss_scale: float32 [1], replicated, may hold values from 16 to 64
Outputs:
- hvp: float32 [2560, 7168], P('dp', 'tensor')
- rayleigh: float32 [1], replicated
The draws below stay inside these ranges and needn't reach their ends.
All inputs are finite; a program needn't handle non-finite values.
Results may differ from the reference program's by a relative error of at most 0.017.
Values may be sent and summed in bfloat16 or wider, within the bound.
No kernel may reach another device: no remote copies, remote signals or barrier semaphores. Data moves between devices by JAX's collectives and lax.ppermute only.
A program may use at most 128 MiB of HBM per device.

```python
import math
import jax
import jax.numpy as jnp
from jax import lax

D = 2560
FF = 7168
TOK_DEV = 256
MICRO = 4
TOKENS = 8192
MB_TOK = 2048
N_DP = 32


def set_ends(result, rng, least, largest):
    longest = result.shape.index(max(result.shape))
    spots = []
    for shift in (0, 1):
        where = [jax.random.randint(jax.random.fold_in(rng, axis), (), 0, length) for axis, length in enumerate(result.shape)]
        where[longest] = (where[longest] + shift) % result.shape[longest]
        spots.append(tuple(where))
    return result.at[spots[0]].set(least).at[spots[1]].set(largest)


def block_levels(key, shape, cuts, smallest, largest):
    def one(axis_at, shards_of):
        heights = jax.random.uniform(jax.random.fold_in(jax.random.fold_in(key, 6), axis_at), (shards_of,), jnp.float32, smallest / len(cuts), largest / len(cuts))
        return jnp.repeat(jnp.exp(heights), shape[axis_at] // shards_of).reshape((-1,) + (1,) * (len(shape) - axis_at - 1))

    gain = one(*cuts[0])
    for cut in cuts[1:]:
        gain = gain * one(*cut)
    return gain


def gaussian(rng, shape, spread, most, split=(), held_as=jnp.bfloat16):
    array = jax.random.normal(rng, shape, jnp.float32) * spread
    if len(split) > 0:
        array = block_levels(rng, shape, split, -0.22, 0.18) * array
    return jnp.clip(array, min=-most, max=most).astype(held_as)


def setup_inputs(seed: int = 0) -> dict:
    splits = jax.random.split(jax.random.key(seed), 10)
    tokens = gaussian(splits[0], (TOKENS, D), 1.0, 6.0, ((0, 32),))
    target = gaussian(splits[1], (TOKENS, D), 1.0, 6.0, ((0, 32),))
    norm_gain = jnp.clip(1.0 + 0.15 * jax.random.normal(splits[2], (D,), jnp.float32), 0.25, 1.75)
    gate_weight = gaussian(splits[3], (D, FF), D ** -0.5, 0.125, ((0, 32), (1, 8)))
    up_weight = gaussian(splits[4], (D, FF), D ** -0.5, 0.125, ((0, 32), (1, 8)))
    down_weight = gaussian(splits[5], (FF, D), FF ** -0.5, 0.0625, ((0, 8), (1, 32)))
    tangent = gaussian(splits[6], (D, FF), D ** -0.5, 0.125, ((0, 32), (1, 8)))
    lengths = set_ends(jax.random.randint(splits[7], (MICRO,), MB_TOK // 4, MB_TOK + 1), jax.random.fold_in(splits[7], 1), MB_TOK // 4, MB_TOK).astype(jnp.int32)
    loss_scale = jnp.clip(jnp.exp(jax.random.uniform(splits[8], (1,), jnp.float32, math.log(16.0), math.log(64.0))), 16.0, 64.0)
    return {"tokens": tokens, "target": target, "norm_gain": norm_gain, "gate_weight": gate_weight, "up_weight": up_weight, "down_weight": down_weight, "tangent": tangent, "lengths": lengths, "loss_scale": loss_scale}


def reference(tokens, target, norm_gain, gate_weight, up_weight, down_weight, tangent, lengths, loss_scale):
    stream = tokens.astype(jnp.float32)
    mean_sq = lax.optimization_barrier(jnp.mean(stream * stream, axis=-1, keepdims=True))
    normed = (stream * lax.rsqrt(mean_sq + 1e-06) * norm_gain[None, :]).astype(jnp.bfloat16)
    gate_pre = jnp.dot(normed, gate_weight, preferred_element_type=jnp.float32)
    up_pre = jnp.dot(normed, up_weight, preferred_element_type=jnp.float32)
    gate_tan = jnp.dot(normed, tangent, preferred_element_type=jnp.float32)
    sigma = jax.nn.sigmoid(gate_pre)
    slope = sigma * (1.0 + gate_pre * (1.0 - sigma))
    bend = sigma * (1.0 - sigma) * (2.0 + gate_pre * (1.0 - 2.0 * sigma))
    hidden = (gate_pre * sigma * up_pre).astype(jnp.bfloat16)
    hidden_tan = (slope * gate_tan * up_pre).astype(jnp.bfloat16)
    output = stream + jnp.dot(hidden, down_weight, preferred_element_type=jnp.float32)
    output_tan = jnp.dot(hidden_tan, down_weight, preferred_element_type=jnp.float32)
    position = jnp.arange(TOKENS, dtype=jnp.int32)
    micro_id = position // MB_TOK
    offset = position - micro_id * MB_TOK
    onehot = micro_id[:, None] == jnp.arange(MICRO, dtype=jnp.int32)[None, :]
    live_len = lax.optimization_barrier(jnp.sum(jnp.where(onehot, lengths[None, :], 0), axis=1))
    weight = jnp.where(offset < live_len, loss_scale[0] / live_len.astype(jnp.float32), jnp.float32(0.0))
    grad_out = (weight[:, None] * (output - target.astype(jnp.float32))).astype(jnp.bfloat16)
    grad_tan = (weight[:, None] * output_tan).astype(jnp.bfloat16)
    dims = (((1,), (1,)), ((), ()))
    grad_hid = lax.dot_general(grad_out, down_weight, dims, preferred_element_type=jnp.float32)
    hess_hid = lax.dot_general(grad_tan, down_weight, dims, preferred_element_type=jnp.float32)
    hess_pre = (hess_hid * up_pre * slope + grad_hid * up_pre * bend * gate_tan).astype(jnp.bfloat16)
    normed_blocks = normed.reshape(N_DP, TOK_DEV, D)
    hess_blocks = hess_pre.reshape(N_DP, TOK_DEV, FF)

    def accumulate(total, pair):
        left, right = pair
        product = lax.dot_general(left, right, (((0,), (0,)), ((), ())), preferred_element_type=jnp.float32)
        product = lax.optimization_barrier(product.astype(jnp.bfloat16)).astype(jnp.float32)
        return (total + product, None)
    hvp, _ = lax.scan(accumulate, jnp.zeros((D, FF), jnp.float32), (normed_blocks, hess_blocks))
    tangent_f = tangent.astype(jnp.float32)
    rayleigh = jnp.sum(tangent_f * hvp) / jnp.sum(tangent_f * tangent_f)
    return (hvp, rayleigh.reshape(1))
```

```python
import jax
import jax.numpy as jnp
from jax import lax
from jax.sharding import Mesh
from jax.sharding import PartitionSpec as P

DP = ("zh", "y", "c")
TENSOR = ("zl", "x")
SIZE = {"zh": 4, "y": 4, "c": 2, "zl": 2, "x": 4}
OFFSETS = (0, -1, 1, 2)


def shift(value, axis, step):
    n = SIZE[axis]
    return lax.ppermute(value, axis, [(i, (i + step) % n) for i in range(n)])


def onward(value, axis):
    n = SIZE[axis]
    pairs = [(i * 2 + c, ((i + (1 if c == 0 else -1)) % n) * 2 + c) for i in range(n) for c in range(2)]
    return lax.ppermute(value, (axis, "c"), pairs)


def four(value, axis):
    below, above = shift(value, axis, 1), shift(value, axis, -1)
    first = lax.axis_index("c") == 0
    return [value, below, above, onward(jnp.where(first, below, above), axis)]


def token_weights(position, micro_len, lengths, loss_scale):
    micro_id = position // micro_len
    offset = position - micro_id * micro_len
    onehot = micro_id[:, None] == jnp.arange(lengths.shape[0], dtype=jnp.int32)[None, :]
    live_len = jnp.sum(jnp.where(onehot, lengths[None, :], 0), axis=1)
    return jnp.where(
        offset < live_len, loss_scale[0] / live_len.astype(jnp.float32), jnp.float32(0.0)
    )


def dot(a, b, ca, cb):
    return lax.dot_general(a, b, (((ca,), (cb,)), ((), ())), preferred_element_type=jnp.float32)


def everyone(value):
    for axis in ("c", "zl", "x", "y", "zh"):
        value = sum([shift(value, axis, s) for s in range(1, SIZE[axis])], value)
    return value


def shards(
    tokens, target, norm_gain, gate_weight, up_weight, down_weight, tangent, lengths, loss_scale
):
    bf, f32 = jnp.bfloat16, jnp.float32
    rows, width = tokens.shape
    part, hid = gate_weight.shape
    half = width // 2
    zh, y, c, zl, x = (lax.axis_index(a) for a in ("zh", "y", "c", "zl", "x"))

    w = jnp.concatenate([gate_weight, up_weight, tangent], axis=1)
    down = lax.all_gather(down_weight, DP, axis=1, tiled=True)

    piece = rows // 8
    order = jnp.stack([(zl ^ (r // 4)) * 4 + (x + r % 4) % 4 for r in range(8)])
    mine = order[0] * piece
    toks = jnp.take(tokens.reshape(8, piece, width), order, axis=0).reshape(rows, width)
    stream = toks.astype(f32)
    mean_sq = jnp.mean(stream * stream, axis=-1, keepdims=True)
    normed = (stream * lax.rsqrt(mean_sq + 1e-06) * norm_gain[None, :]).astype(bf)
    lines = normed.T.reshape(32, part, rows)

    def block(dz, dy, dc):
        return ((zh + dz) % 4) * 8 + ((y + dy) % 4) * 2 + (c ^ dc)

    into = jnp.stack([block(dz, dy, dc) for dz in OFFSETS for dc in (0, 1) for dy in OFFSETS])
    outof = jnp.stack([block(dz, dy, dc) for dc in (1, 0) for dy in (1, 2, 3, 0) for dz in (1, 2, 3, 0)])
    n_in = jnp.take(lines, into, axis=0).reshape(width, rows)
    n_out = jnp.take(lines, outof, axis=0).reshape(width, rows)

    pre = jnp.zeros((rows, 3 * hid), f32)
    four_z = four(w, "zh")
    step = 4 * part
    for i, value in enumerate(four_z):
        own = jnp.concatenate(four(value, "y"), axis=0)
        other = shift(own, "c", 1)
        at = 2 * i * step
        pre = pre + dot(n_in[at : at + step], own, 0, 0)
        pre = pre + dot(n_in[at + step : at + 2 * step], other, 0, 0)
    gate_pre, up_pre, gate_tan = pre[:, :hid], pre[:, hid : 2 * hid], pre[:, 2 * hid :]

    sigma = jax.nn.sigmoid(gate_pre)
    slope = sigma * (1.0 + gate_pre * (1.0 - sigma))
    bend = sigma * (1.0 - sigma) * (2.0 + gate_pre * (1.0 - 2.0 * sigma))
    hidden = (gate_pre * sigma * up_pre).astype(bf)
    hidden_tan = (slope * gate_tan * up_pre).astype(bf)
    both = jnp.concatenate(
        [hidden.reshape(8, piece, hid), hidden_tan.reshape(8, piece, hid)], axis=1
    ).reshape(2 * rows, hid)

    wide = 2 * piece
    left = dot(both, down[:, :half], 1, 0).astype(bf).reshape(2, 4, wide, half)
    right = dot(both, down[:, half:], 1, 0).astype(bf).reshape(2, 4, wide, half)
    got_z = shift(right[1], "zl", 1)
    got_x = [shift(left[:, d], "x", d) for d in (1, 2, 3)]
    right_z = (right[0].astype(f32) + got_z.astype(f32)).astype(bf)
    got_zx = [shift(right_z[d], "x", d) for d in (1, 2, 3)]
    left_x = left[:, 0].astype(f32) + sum(g.astype(f32) for g in got_x)
    got_xz = shift(left_x[1].astype(bf), "zl", 1)
    left_sum = left_x[0] + got_xz.astype(f32)
    right_sum = right_z[0].astype(f32) + sum(g.astype(f32) for g in got_zx)

    micro_len = rows * 32 // lengths.shape[0]
    position = ((zh * 4 + y) * 2 + c) * rows + mine + jnp.arange(piece, dtype=jnp.int32)
    weight = token_weights(position, micro_len, lengths, loss_scale)[:, None]
    start = stream[:piece] - lax.dynamic_slice_in_dim(target, mine, piece, 0).astype(f32)

    def grads(total, cols):
        out = weight * (start[:, cols] + total[:piece])
        return jnp.concatenate([out, weight * total[piece:]], axis=0).astype(bf)

    left_g, right_g = grads(left_sum, slice(0, half)), grads(right_sum, slice(half, width))
    left_gz = jnp.stack([left_g, shift(left_g, "zl", 1)])
    right_gx = jnp.stack([right_g] + [shift(right_g, "x", -d) for d in (1, 2, 3)])
    left_gx = [left_gz] + [shift(left_gz, "x", -d) for d in (1, 2, 3)]
    right_gz = [right_gx, shift(right_gx, "zl", 1)]
    left_all = jnp.concatenate([left_gx[d][k] for k in (0, 1) for d in range(4)], axis=0)
    right_all = jnp.concatenate(right_gz, axis=0).reshape(2 * rows, half)
    hid_grads = dot(left_all, down[:, :half], 1, 1) + dot(right_all, down[:, half:], 1, 1)
    hid_grads = hid_grads.reshape(8, 2, piece, hid)
    grad_hid = hid_grads[:, 0].reshape(rows, hid)
    hess_hid = hid_grads[:, 1].reshape(rows, hid)
    hess_pre = (hess_hid * up_pre * slope + grad_hid * up_pre * bend * gate_tan).astype(bf)

    tangent_f = tangent.astype(f32)
    curvature = jnp.sum(gate_tan * hess_pre.astype(f32))
    squares = jnp.sum(tangent_f * tangent_f)
    lane = lax.broadcasted_iota(jnp.int32, (8, 128), 0)
    totals = everyone(jnp.where(lane == 0, curvature, squares))
    rayleigh = (totals[0, 0] / totals[1, 0]).reshape(1)

    pieces = []
    for lo, hi in ((0, 512), (512, hid)):
        rhs = hess_pre[:, lo:hi]
        other = shift(dot(n_out[: width // 2], rhs, 1, 0).astype(bf), "c", 1)
        own = dot(n_out[width // 2 :], rhs, 1, 0).astype(bf)
        chip = (own.astype(f32) + other.astype(f32)).astype(bf).reshape(4, 4 * part, hi - lo)
        got = [shift(chip[d - 1], "y", d) for d in (1, 2, 3)]
        line = (chip[3].astype(f32) + sum(g.astype(f32) for g in got)).astype(bf)
        line = line.reshape(4, part, hi - lo)
        got = [shift(line[d - 1], "zh", d) for d in (1, 2, 3)]
        pieces.append(line[3].astype(f32) + sum(g.astype(f32) for g in got))
    return jnp.concatenate(pieces, axis=1), rayleigh


def solution(mesh):
    torus = Mesh(mesh.devices.reshape(4, 4, 2, 2, 4), DP + TENSOR)
    return jax.shard_map(
        shards,
        mesh=torus,
        in_specs=(
            P(DP, None), P(DP, None), P(), P(DP, TENSOR), P(DP, TENSOR), P(TENSOR, DP),
            P(DP, TENSOR), P(), P(),
        ),
        out_specs=(P(DP, TENSOR), P()),
        check_vma=False,
    )
```

```python
import jax
import jax.numpy as jnp
from jax import lax
from jax.sharding import Mesh
from jax.sharding import PartitionSpec as P


DP = ("zh", "y", "c")
TENSOR = ("zl", "x")
SIZE = {"zh": 4, "y": 4, "c": 2, "zl": 2, "x": 4}


def shift(value, axis, step):
    n = SIZE[axis]
    return lax.ppermute(value, axis, [(i, (i + step) % n) for i in range(n)])


def onward(value, axis):
    n = SIZE[axis]
    pairs = [(i * 2 + c, ((i + (1 if c == 0 else -1)) % n) * 2 + c) for i in range(n) for c in range(2)]
    return lax.ppermute(value, (axis, "c"), pairs)


def exchange(value, axes):
    return lax.all_to_all(value, axes, 0, 0, tiled=True)


def to_all(value, axes, n):
    return exchange(jnp.broadcast_to(value[None], (n,) + value.shape), axes)


def token_weights(position, micro_len, lengths, loss_scale):
    micro_id = position // micro_len
    offset = position - micro_id * micro_len
    onehot = micro_id[:, None] == jnp.arange(lengths.shape[0], dtype=jnp.int32)[None, :]
    live_len = jnp.sum(jnp.where(onehot, lengths[None, :], 0), axis=1)
    return jnp.where(
        offset < live_len, loss_scale[0] / live_len.astype(jnp.float32), jnp.float32(0.0)
    )


def dot(a, b, ca, cb):
    return lax.dot_general(a, b, (((ca,), (cb,)), ((), ())), preferred_element_type=jnp.float32)


def cat(*parts):
    return jnp.concatenate(parts, axis=0)


def swapped(*parts):
    own = lax.optimization_barrier(cat(*parts))
    return own, shift(own, "c", 1)


def added(value):
    return jnp.sum(value.astype(jnp.float32), axis=0)


G = ((0, 0), (0, -1), (0, 1), (0, 2))
AB = (
    (-1, 0), (1, 0), (-1, -1), (1, -1), (-1, 1), (1, 1),
    (2, 0), (2, -1), (2, 1),
)
CE = ((-1, 2), (1, 2), (2, 2))


def shards(
    tokens, target, norm_gain, gate_weight, up_weight, down_weight, tangent, lengths, loss_scale
):
    bf, f32 = jnp.bfloat16, jnp.float32
    rows, width = tokens.shape
    part, hid = gate_weight.shape
    half = width // 2
    piece = rows // 8
    wide = 2 * piece
    zh, y, c, zl, x = (lax.axis_index(a) for a in ("zh", "y", "c", "zl", "x"))
    first = c == 0

    def block(dz, dy, dc):
        return ((zh + dz) & 3) * 8 + ((y + dy) & 3) * 2 + (c ^ dc)

    w = lax.optimization_barrier(jnp.concatenate([gate_weight, up_weight, tangent], axis=1))
    d = down_weight.T
    w_zp, w_zm = shift(w, "zh", 1), shift(w, "zh", -1)
    w_yp, w_ym = shift(w, "y", 1), shift(w, "y", -1)
    w_y2 = onward(jnp.where(first, w_yp, w_ym), "y")
    b = onward(jnp.where(first, w_zp, w_zm), "zh")
    a = cat(w_zp, w_zm)
    a_yp, a_ym = shift(a, "y", 1), shift(a, "y", -1)
    d_yp, d_ym = shift(d, "y", 1), shift(d, "y", -1)
    d_0 = cat(d, d_yp, d_ym, onward(jnp.where(first, d_yp, d_ym), "y"))
    d_0 = lax.optimization_barrier(d_0)
    d_zp, d_zm = shift(d_0, "zh", 1), shift(d_0, "zh", -1)
    b_yp, b_ym = shift(b, "y", 1), shift(b, "y", -1)
    g = lax.optimization_barrier(cat(*swapped(w, w_yp, w_ym, w_y2)))
    a_y2 = jnp.where(first, a_yp, a_ym)
    d_zp, d_zm, _ = lax.optimization_barrier((d_zp, d_zm, a_y2))
    a_y2 = onward(a_y2, "y")
    b_y2 = onward(jnp.where(first, b_yp, b_ym), "y")
    ab_own, ab_other = swapped(a, a_yp, a_ym, b, b_yp, b_ym)
    ce_own, ce_other = swapped(a_y2, b_y2)
    d_z2 = onward(jnp.where(first, d_zp, d_zm), "zh")
    down = lax.optimization_barrier(cat(*swapped(d_0, d_zp, d_zm, d_z2)))
    down_order = jnp.stack(
        [block(dz, dy, dc) for dc in (0, 1) for dz in (0, -1, 1, 2) for dy in (0, -1, 1, 2)]
    )

    stream = tokens.astype(f32)
    mean_sq = jnp.mean(stream * stream, axis=-1, keepdims=True)
    normed = (stream * lax.rsqrt(mean_sq + 1e-06) * norm_gain[None, :]).astype(bf)
    lines = normed.T.reshape(32, part, rows)
    into = jnp.stack([block(dz, dy, dc) for group in (G, AB, CE) for dc in (0, 1) for dz, dy in group])
    n_in = jnp.take(lines, into, axis=0).reshape(width, rows)
    outof = [jnp.stack([block(dz - zh, dy, dc) for dy in (1, 2, 3, 0) for dz in range(4)]) for dc in (0, 1)]
    n_own, n_other = (jnp.take(lines, at, axis=0).reshape(half, rows) for at in outof)
    mine = (zl * 4 + x) * piece
    start = lax.dynamic_slice_in_dim(tokens, mine, piece, 0).astype(f32)
    start = start - lax.dynamic_slice_in_dim(target, mine, piece, 0).astype(f32)
    start = jnp.take(start.T.reshape(32, part, piece), down_order, axis=0).reshape(width, piece).T
    micro_len = rows * 32 // lengths.shape[0]
    position = ((zh * 4 + y) * 2 + c) * rows + mine + jnp.arange(piece, dtype=jnp.int32)
    weight = token_weights(position, micro_len, lengths, loss_scale)[:, None]
    tangent_f = tangent.astype(f32)
    squares = jnp.sum(tangent_f * tangent_f)

    pre, at = 0.0, 0
    for group in (g, ab_own, ab_other, ce_own, ce_other):
        pre = lax.optimization_barrier(pre + dot(n_in[at : at + group.shape[0]], group, 0, 0))
        at += group.shape[0]
    gate_pre, up_pre, gate_tan = pre[:, :hid], pre[:, hid : 2 * hid], pre[:, 2 * hid :]

    sigma = jax.nn.sigmoid(gate_pre)
    slope = sigma * (1.0 + gate_pre * (1.0 - sigma))
    bend = sigma * (1.0 - sigma) * (2.0 + gate_pre * (1.0 - 2.0 * sigma))
    hidden = (gate_pre * sigma * up_pre).astype(bf)
    hidden_tan = (slope * gate_tan * up_pre).astype(bf)
    both = jnp.concatenate(
        [hidden.reshape(8, piece, hid), hidden_tan.reshape(8, piece, hid)], axis=1
    ).reshape(2 * rows, hid)

    partial = dot(both, down, 1, 1).astype(bf)
    total = added(exchange(partial.reshape(8, wide, width), TENSOR))
    grads = cat(weight * (start + total[:piece]), weight * total[piece:]).astype(bf)
    grads = to_all(grads, TENSOR, 8).reshape(2 * rows, width)
    hid_grads = dot(grads, down, 1, 0)
    hid_grads = hid_grads.reshape(8, 2, piece, hid)
    grad_hid = hid_grads[:, 0].reshape(rows, hid)
    hess_hid = hid_grads[:, 1].reshape(rows, hid)
    hess_pre = (hess_hid * up_pre * slope + grad_hid * up_pre * bend * gate_tan).astype(bf)

    curvature = jnp.sum(gate_tan * hess_pre.astype(f32))
    lane = lax.broadcasted_iota(jnp.int32, (8, 128), 0)
    totals = added(to_all(jnp.where(lane == 0, curvature, squares), ("c",) + TENSOR, 16))
    totals = added(to_all(totals, ("zh", "y"), 16))
    rayleigh = (totals[0, 0] / totals[1, 0]).reshape(1)

    other = shift(dot(n_other, hess_pre, 1, 0).astype(bf), "c", 1)
    own = dot(n_own, hess_pre, 1, 0).astype(bf)
    chip = (own.astype(f32) + other.astype(f32)).astype(bf).reshape(4, 4 * part, hid)
    got = [shift(chip[s - 1], "y", s) for s in (1, 2, 3)]
    line = (chip[3].astype(f32) + sum(g.astype(f32) for g in got)).astype(bf).reshape(4, part, hid)
    return added(exchange(line, "zh")), rayleigh


def solution(mesh):
    torus = Mesh(mesh.devices.reshape(4, 4, 2, 2, 4), DP + TENSOR)
    return jax.shard_map(
        shards,
        mesh=torus,
        in_specs=(
            P(DP, None), P(DP, None), P(), P(DP, TENSOR), P(DP, TENSOR), P(TENSOR, DP),
            P(DP, TENSOR), P(), P(),
        ),
        out_specs=(P(DP, TENSOR), P()),
        check_vma=False,
    )
```

```python
import jax
import jax.numpy as jnp
import numpy as np
from jax import lax
from jax.sharding import Mesh
from jax.sharding import PartitionSpec as P


DP = ("zh", "y", "c")
TENSOR = ("zl", "x")
SIZE = {"zh": 4, "y": 4, "c": 2, "zl": 2, "x": 4}


def shift(value, axis, step):
    n = SIZE[axis]
    return lax.ppermute(value, axis, [(i, (i + step) % n) for i in range(n)])


def onward(value, axis):
    n = SIZE[axis]
    pairs = [(i * 2 + c, ((i + (1 if c == 0 else -1)) % n) * 2 + c) for i in range(n) for c in range(2)]
    return lax.ppermute(value, (axis, "c"), pairs)


def exchange(value, axes):
    return lax.all_to_all(value, axes, 0, 0, tiled=True)


def to_all(value, axes, n):
    return exchange(jnp.broadcast_to(value[None], (n,) + value.shape), axes)


def token_weights(position, micro_len, lengths, loss_scale):
    micro_id = position // micro_len
    offset = position - micro_id * micro_len
    onehot = micro_id[:, None] == jnp.arange(lengths.shape[0], dtype=jnp.int32)[None, :]
    live_len = jnp.sum(jnp.where(onehot, lengths[None, :], 0), axis=1)
    return jnp.where(
        offset < live_len, loss_scale[0] / live_len.astype(jnp.float32), jnp.float32(0.0)
    )


def dot(a, b, ca, cb):
    return lax.dot_general(a, b, (((ca,), (cb,)), ((), ())), preferred_element_type=jnp.float32)


def cat(*parts):
    return jnp.concatenate(parts, axis=0)


def swapped(*parts):
    own = lax.optimization_barrier(cat(*parts))
    return own, shift(own, "c", 1)


def added(value):
    return jnp.sum(value.astype(jnp.float32), axis=0)


OFFSETS = (0, -1, 1, 2)
G = ((0, 0), (0, -1), (0, 1), (0, 2))
AB = (
    (-1, 0), (1, 0), (-1, -1), (1, -1), (-1, 1), (1, 1),
    (2, 0), (2, -1), (2, 1),
)
CE = ((-1, 2), (1, 2), (2, 2))


def shards(
    tokens, target, norm_gain, gate_weight, up_weight, down_weight, tangent, lengths, loss_scale
):
    bf, f32 = jnp.bfloat16, jnp.float32
    rows, width = tokens.shape
    part, hid = gate_weight.shape
    half = width // 2
    piece = rows // 8
    wide = 2 * piece
    zh, y, c, zl, x = (lax.axis_index(a) for a in ("zh", "y", "c", "zl", "x"))
    first = c == 0

    def blocks(places, from_z, from_y):
        dz, dy, dc = np.array(places, np.int32).T
        return ((from_z + dz) & 3) * 8 + ((from_y + dy) & 3) * 2 + (c ^ dc)

    w = lax.optimization_barrier(jnp.concatenate([gate_weight, up_weight, tangent], axis=1))
    d = down_weight.T
    w_zp, w_zm = shift(w, "zh", 1), shift(w, "zh", -1)
    w_yp, w_ym = shift(w, "y", 1), shift(w, "y", -1)
    w_y2 = onward(jnp.where(first, w_yp, w_ym), "y")
    b = onward(jnp.where(first, w_zp, w_zm), "zh")
    a = cat(w_zp, w_zm)
    a_yp, a_ym = shift(a, "y", 1), shift(a, "y", -1)
    d_0 = lax.optimization_barrier(to_all(d, "y", 4).reshape(4 * part, hid))
    d_zp, d_zm = shift(d_0, "zh", 1), shift(d_0, "zh", -1)
    b_yp, b_ym = shift(b, "y", 1), shift(b, "y", -1)
    g = lax.optimization_barrier(cat(*swapped(w, w_yp, w_ym, w_y2)))
    a_y2 = jnp.where(first, a_yp, a_ym)
    d_zp, d_zm, _ = lax.optimization_barrier((d_zp, d_zm, a_y2))
    a_y2 = onward(a_y2, "y")
    b_y2 = onward(jnp.where(first, b_yp, b_ym), "y")
    ab_own, ab_other = swapped(a, a_yp, a_ym, b, b_yp, b_ym)
    ce = lax.optimization_barrier(cat(*swapped(a_y2, b_y2)))
    d_z2 = onward(jnp.where(first, d_zp, d_zm), "zh")
    down = lax.optimization_barrier(cat(*swapped(d_0, d_zp, d_zm, d_z2)))
    down_order = blocks([(dz, dy, dc) for dc in (0, 1) for dz in OFFSETS for dy in range(4)], zh, 0)

    stream = tokens.astype(f32)
    mean_sq = jnp.mean(stream * stream, axis=-1, keepdims=True)
    normed = (stream * lax.rsqrt(mean_sq + 1e-06) * norm_gain[None, :]).astype(bf)
    lines = normed.T.reshape(32, part, rows)
    into = blocks([(dz, dy, dc) for group in (G, AB, CE) for dc in (0, 1) for dz, dy in group], zh, y)
    n_in = jnp.take(lines, into, axis=0).reshape(width, rows)
    outof = blocks([(dz, dy, dc) for dc in (1, 0) for dy in (1, 2, 3, 0) for dz in range(4)], 0, y)
    n_out = jnp.take(lines, outof, axis=0).reshape(width, rows)
    mine = (zl * 4 + x) * piece
    start = lax.dynamic_slice_in_dim(tokens, mine, piece, 0).astype(f32)
    start = start - lax.dynamic_slice_in_dim(target, mine, piece, 0).astype(f32)
    start = jnp.take(start.T.reshape(32, part, piece), down_order, axis=0).reshape(width, piece).T
    micro_len = rows * 32 // lengths.shape[0]
    position = ((zh * 4 + y) * 2 + c) * rows + mine + jnp.arange(piece, dtype=jnp.int32)
    weight = token_weights(position, micro_len, lengths, loss_scale)[:, None]
    tangent_f = tangent.astype(f32)
    squares = jnp.sum(tangent_f * tangent_f)

    pre, at = 0.0, 0
    for group in (g, ab_own, ab_other, ce):
        pre = lax.optimization_barrier(pre + dot(n_in[at : at + group.shape[0]], group, 0, 0))
        at += group.shape[0]
    gate_pre, up_pre, gate_tan = pre[:, :hid], pre[:, hid : 2 * hid], pre[:, 2 * hid :]

    sigma = jax.nn.sigmoid(gate_pre)
    slope = sigma * (1.0 + gate_pre * (1.0 - sigma))
    bend = sigma * (1.0 - sigma) * (2.0 + gate_pre * (1.0 - 2.0 * sigma))
    hidden = (gate_pre * sigma * up_pre).astype(bf)
    hidden_tan = (slope * gate_tan * up_pre).astype(bf)
    both = jnp.concatenate(
        [hidden.reshape(8, piece, hid), hidden_tan.reshape(8, piece, hid)], axis=1
    ).reshape(2 * rows, hid)

    partial = dot(both, down, 1, 1).astype(bf)
    total = added(exchange(partial.reshape(8, wide, width), TENSOR))
    grads = cat(weight * (start + total[:piece]), weight * total[piece:]).astype(bf)
    grads = to_all(grads, TENSOR, 8).reshape(2 * rows, width)
    hid_grads = dot(grads, down, 1, 0)
    hid_grads = hid_grads.reshape(8, 2, piece, hid)
    grad_hid = hid_grads[:, 0].reshape(rows, hid)
    hess_hid = hid_grads[:, 1].reshape(rows, hid)
    hess_pre = (hess_hid * up_pre * slope + grad_hid * up_pre * bend * gate_tan).astype(bf)

    curvature = jnp.sum(gate_tan * hess_pre.astype(f32))
    lane = lax.broadcasted_iota(jnp.int32, (8, 128), 0)
    totals = added(to_all(jnp.where(lane == 0, curvature, squares), ("c",) + TENSOR, 16))
    totals = added(to_all(totals, ("zh", "y"), 16))
    rayleigh = (totals[0, 0] / totals[1, 0]).reshape(1)

    product = dot(n_out, hess_pre, 1, 0).astype(bf)
    other, own = shift(product[:half], "c", 1), product[half:]
    chip = (own.astype(f32) + other.astype(f32)).astype(bf).reshape(4, 4 * part, hid)
    got = [shift(chip[s - 1], "y", s) for s in (1, 2, 3)]
    line = (chip[3].astype(f32) + sum(g.astype(f32) for g in got)).astype(bf).reshape(4, part, hid)
    return added(exchange(line, "zh")), rayleigh


def solution(mesh):
    torus = Mesh(mesh.devices.reshape(4, 4, 2, 2, 4), DP + TENSOR)
    return jax.shard_map(
        shards,
        mesh=torus,
        in_specs=(
            P(DP, None), P(DP, None), P(), P(DP, TENSOR), P(DP, TENSOR), P(TENSOR, DP),
            P(DP, TENSOR), P(), P(),
        ),
        out_specs=(P(DP, TENSOR), P()),
        check_vma=False,
    )
```
